8 devices in a mesh: data: 2 (over z, y), model: 4 (over x, core).
Axes of the slice: x: 2, y: 2, z: 1, core: 2. Of those that a mesh axis runs over, the one named last changes fastest.
Arguments:
- hidden: bfloat16 [8192, 5120], P('data', 'model')
- unembed: bfloat16 [32000, 5120], P('model', 'data')
- draft_ids: int32 [8192], P('data')
- q_prob: float32 [8192], P('data')
Outputs:
- output 1: float32 [8192], P('data')
- output 2: float32 [8192], P('data')
All inputs are finite; a program needn't handle non-finite values.
Results may differ from the reference program's by a relative error of at most 0.001.
Values are sent between devices in bfloat16 or wider.
A program may use at most 1 GiB of HBM per device.

```python
import math
import jax
import jax.numpy as jnp
from jax import lax

VOCAB = 32000
WIDTH = 5120
ROWS = 8192
ROW_BLOCK = 64


def setup_inputs(seed: int = 0) -> dict:
    base_key = jax.random.key(seed)
    k_hid, k_wt, k_draft, k_prob = jax.random.split(base_key, 4)
    hidden = jax.random.normal(k_hid, (ROWS, WIDTH), jnp.float32).astype(jnp.bfloat16)
    unembed = (jax.random.normal(k_wt, (VOCAB, WIDTH), jnp.float32) * WIDTH ** -0.5).astype(jnp.bfloat16)
    draft_ids = jax.random.randint(k_draft, (ROWS,), 0, VOCAB, jnp.int32).at[0].set(VOCAB - 1)
    log_q = -math.log(VOCAB) - 0.5 + jax.random.uniform(k_prob, (ROWS,), jnp.float32, -1.0, 1.0)
    q_prob = jnp.exp(log_q)
    return {"hidden": hidden, "unembed": unembed, "draft_ids": draft_ids, "q_prob": q_prob}


def reference(hidden, unembed, draft_ids, q_prob):
    blocks = ROWS // ROW_BLOCK
    vocab_ids = jnp.arange(VOCAB, dtype=jnp.int32)[None, :]

    def one_block(block_in):
        h_blk, d_blk = block_in
        logits = jnp.dot(h_blk, unembed.T, preferred_element_type=jnp.float32)
        row_max = jnp.max(logits, axis=1)
        log_sum = row_max + jnp.log(jnp.sum(jnp.exp(logits - row_max[:, None]), axis=1))
        picked = jnp.sum(jnp.where(vocab_ids == d_blk[:, None], logits, 0.0), axis=1)
        return picked - log_sum

    log_prob = lax.map(one_block, (hidden.reshape(blocks, ROW_BLOCK, WIDTH), draft_ids.reshape(blocks, ROW_BLOCK))).reshape(ROWS)
    accept = jnp.minimum(1.0, jnp.exp(log_prob) / q_prob)
    return log_prob, accept
```

```python
import functools

import jax
import jax.numpy as jnp
from jax import lax
from jax.experimental import pallas as pl
from jax.experimental.pallas import tpu as pltpu
from jax.sharding import PartitionSpec as P

MESH = pl.DeviceIdType.MESH
WC = 400
R1 = 512
PIECE = 128
R2 = 256


def _kernel(rows, quarter, shard, half, h_ref, w_ref, d_ref, q_ref, lp_ref, ac_ref, ha_ref,
            wv, hb, dv, st1, sta, stb, own_sem, ld_sem, d_sem, w_ss, w_rs, y_ss, y_rs,
            x1_ss, x1_rs, d1_ss, d1_rs, f1_ss, f1_rs, x2_ss, x2_rs, d2_ss, d2_rs, f2_ss, f2_rs,
            sa_ss, sa_rs, sb_ss, sb_rs):
    y = lax.axis_index("data")
    m = lax.axis_index("model")
    x = m // 2
    c = m % 2
    oy = 1 - y
    ox = 1 - x
    oc = 1 - c
    me_id = (y, m)
    dev_y = (oy, m)
    dev_x = (y, ox * 2 + c)
    dev_d = (y, x * 2 + oc)
    vocab = shard // 2
    base = m * shard + y * vocab
    n_wc = vocab // WC
    n_rb = rows // R1
    n_pc = rows // PIECE
    n_b2 = rows // R2

    def col(p):
        return pl.ds(pl.multiple_of(p * quarter, 128), quarter)

    def whalf(hh):
        return pl.ds(pl.multiple_of(lax.rem(hh + x, 2) * half, 128), half)

    def peer(k):
        kx, kc = k // 2, k % 2
        return lax.rem(x + kx, 2) * 2 + lax.rem(c + kc, 2)

    bar = pltpu.get_barrier_semaphore()
    for dy in range(2):
        for k in range(4):
            if dy or k:
                pl.semaphore_signal(bar, 1, device_id=(lax.rem(y + dy, 2), peer(k)), device_id_type=MESH)
    pl.semaphore_wait(bar, 7)

    def rcopy(src, dst, ss, rs, dev):
        return pltpu.make_async_remote_copy(src, dst, ss, rs, device_id=dev, device_id_type=MESH)

    def w_copy(j):
        return rcopy(w_ref.at[pl.ds(pl.multiple_of(oy * vocab + j * WC, 16), WC)],
                     wv.at[pl.ds(pl.multiple_of(j * WC, 16), WC), whalf(y)], w_ss.at[j], w_rs.at[j], dev_y)

    def w_wait(j):
        rcopy(w_ref.at[pl.ds(0, WC)], wv.at[pl.ds(pl.multiple_of(j * WC, 16), WC), whalf(oy)],
              w_ss.at[j], w_rs.at[j], dev_y).wait_recv()

    def prow(yy, t):
        return pl.ds(pl.multiple_of(yy * rows + t * PIECE, PIECE), PIECE)

    def y_copy(t):
        return rcopy(h_ref.at[pl.ds(pl.multiple_of(t * PIECE, PIECE), PIECE)], ha_ref.at[prow(y, t), col(c)],
                     y_ss.at[t], y_rs.at[t], dev_y)

    def y_wait(t):
        rcopy(h_ref.at[pl.ds(0, PIECE)], ha_ref.at[prow(oy, t), col(c)], y_ss.at[t], y_rs.at[t], dev_y).wait_recv()

    def rrow(i):
        return pl.ds(pl.multiple_of(y * rows + i * R1, R1), R1)

    def x1_copy(i):
        return rcopy(h_ref.at[pl.ds(pl.multiple_of(i * R1, R1), R1)], ha_ref.at[rrow(i), col(2 + c)],
                     x1_ss.at[i], x1_rs.at[i], dev_x)

    def d1_copy(pos):
        return rcopy(h_ref, ha_ref.at[pl.ds(pl.multiple_of(y * rows, R1), rows), col(pos)],
                     d1_ss, d1_rs, dev_d)

    def f1_copy(i, pos):
        return rcopy(ha_ref.at[rrow(i), col(2 + c)], ha_ref.at[rrow(i), col(2 + pos)],
                     f1_ss.at[i], f1_rs.at[i], dev_d)

    def x2_copy(t):
        return rcopy(ha_ref.at[prow(oy, t), col(c)], ha_ref.at[prow(oy, t), col(2 + c)],
                     x2_ss.at[t], x2_rs.at[t], dev_x)

    def d2_copy(t, pos):
        return rcopy(ha_ref.at[prow(oy, t), col(c)], ha_ref.at[prow(oy, t), col(pos)],
                     d2_ss.at[t], d2_rs.at[t], dev_d)

    def f2_copy(t, pos):
        return rcopy(ha_ref.at[prow(oy, t), col(2 + c)], ha_ref.at[prow(oy, t), col(2 + pos)],
                     f2_ss.at[t], f2_rs.at[t], dev_d)

    def got_y(t):
        y_wait(t)
        x2_copy(t).start()
        d2_copy(t, c).start()

    def got_x(t):
        x2_copy(t).wait_recv()
        f2_copy(t, c).start()

    def start_loop(n, f):
        lax.fori_loop(0, n, lambda i, s: (f(i), s)[1], 0)

    own_w = pltpu.make_async_copy(w_ref.at[pl.ds(pl.multiple_of(y * vocab, 16), vocab)], wv.at[:, whalf(y)], own_sem)
    draft_copy = rcopy(d_ref, dv, d_sem.at[0], d_sem.at[1], dev_y)
    draft_copy.start()
    start_loop(n_wc, lambda j: w_copy(j).start())
    start_loop(n_rb, lambda i: x1_copy(i).start())
    d1_copy(c).start()
    own_w.start()

    def pass_on(i):
        x1_copy(i).wait_recv()
        f1_copy(i, c).start()

    start_loop(n_rb, pass_on)
    d1_copy(oc).wait_recv()
    start_loop(n_rb, lambda i: f1_copy(i, oc).wait_recv())

    def load1(i, s):
        r = pl.ds(pl.multiple_of(i * R1, R1), R1)
        return (
            pltpu.make_async_copy(h_ref.at[r], hb.at[s, :, col(c)], ld_sem.at[s, 0]),
            pltpu.make_async_copy(ha_ref.at[rrow(i), col(oc)], hb.at[s, :, col(oc)], ld_sem.at[s, 1]),
            pltpu.make_async_copy(ha_ref.at[rrow(i), pl.ds(half, half)], hb.at[s, :, pl.ds(half, half)], ld_sem.at[s, 2]),
        )

    def load2(b, s):
        r = pl.ds(pl.multiple_of(oy * rows + b * R2, R2), R2)
        return pltpu.make_async_copy(ha_ref.at[r], hb.at[s, pl.ds(0, R2)], ld_sem.at[s, 0])

    def score(t, v0, hblk, want, st):
        mx, sm, pk = st
        n = want.shape[1]
        wt = wv[pl.ds(pl.multiple_of(v0, 16), t), :]
        lg = lax.dot_general(wt, hblk, (((1,), (1,)), ((), ())), preferred_element_type=jnp.float32)
        lg = lg.reshape(t // 8, 8, n)
        new = jnp.maximum(mx, jnp.max(lg, axis=0))
        sm = sm * jnp.exp(mx - new) + jnp.sum(jnp.exp(lg - new[None]), axis=0)
        ids = lax.broadcasted_iota(jnp.int32, (t // 8, 8, n), 0) * 8 + lax.broadcasted_iota(jnp.int32, (t // 8, 8, n), 1)
        pk = pk + jnp.sum(jnp.where(ids == (want - v0)[None], lg, 0.0), axis=0)
        return new, sm, pk

    def fresh(n):
        return jnp.full((8, n), -jnp.inf, jnp.float32), jnp.zeros((8, n), jnp.float32), jnp.zeros((8, n), jnp.float32)

    def squeeze(st):
        mx, sm, pk = st
        top = jnp.max(mx, axis=0, keepdims=True)
        return top, jnp.sum(sm * jnp.exp(mx - top), axis=0, keepdims=True), jnp.sum(pk, axis=0, keepdims=True)

    def step1(t, v0, i, s):
        @pl.when(v0 == 0)
        def _():
            for k, a in enumerate(fresh(R1)):
                st1[i, k] = a

        want = jnp.broadcast_to(d_ref[:, pl.ds(pl.multiple_of(i * R1, R1), R1)] - base, (8, R1))
        st = score(t, v0, hb[s], want, (st1[i, 0], st1[i, 1], st1[i, 2]))
        for k in range(3):
            st1[i, k] = st[k]

    def fetch1(i, s, last):
        nxt = lax.rem(i + 1, n_rb)

        @pl.when(jnp.logical_not(last))
        def _():
            for cp in load1(nxt, 1 - s):
                cp.start()

        for cp in load1(i, s):
            cp.wait()

    n_pair = (n_wc - 2) // 2
    for cp in load1(0, 0):
        cp.start()
    own_w.wait()

    def pairs(n, carry):
        j, i, s = n // n_rb, lax.rem(n, n_rb), lax.rem(n, 2)

        @pl.when(n == n_pair * n_rb // 2)
        def _():
            start_loop(n_pc, lambda t: y_copy(t).start())

        @pl.when(i == 0)
        def _():
            w_wait(2 * j)
            w_wait(2 * j + 1)

        fetch1(i, s, False)
        step1(2 * WC, j * (2 * WC), i, s)
        return carry

    lax.fori_loop(0, n_pair * n_rb, pairs, 0)

    def singles(n, carry):
        j, i, s = 2 * n_pair + n // n_rb, lax.rem(n, n_rb), lax.rem(n, 2)

        @pl.when(i == 0)
        def _():
            w_wait(j)

        @pl.when(n == n_rb + 4)
        def _():
            got_y(0)

        @pl.when(n == n_rb + 7)
        def _():
            got_y(1)

        fetch1(i, s, n == 2 * n_rb - 1)
        step1(WC, j * WC, i, s)
        return carry

    lax.fori_loop(0, 2 * n_rb, singles, 0)

    slot = y * 4 + m

    def final1(i, carry):
        st = squeeze((st1[i, 0], st1[i, 1], st1[i, 2]))
        for u in range(R1 // R2):
            for k in range(3):
                sta[slot, i * (R1 // R2) + u, k:k + 1, :] = st[k][:, u * R2:(u + 1) * R2]
        return carry

    lax.fori_loop(0, n_rb, final1, 0)

    draft_copy.wait_recv()
    got_x(0)
    got_y(2)
    got_x(1)

    def sa_copy(k, sl):
        return rcopy(sta.at[sl], sta.at[sl], sa_ss.at[k - 1], sa_rs.at[k - 1], (y, peer(k)))

    for k in range(1, 4):
        sa_copy(k, slot).start()

    def arrived(b):
        for u in range(R2 // PIECE):
            t = b * (R2 // PIECE) + u
            d2_copy(t, oc).wait_recv()
            f2_copy(t, oc).wait_recv()

    arrived(0)
    load2(0, 0).start()

    def sb_copy(g, k, b0, nb, sl):
        part = pl.ds(b0, nb)
        return rcopy(stb.at[part], sta.at[sl, part], sb_ss.at[g, k], sb_rs.at[g, k], (oy, peer(k)))

    n_t2 = vocab // (2 * WC)

    def block2(b, carry):
        s = lax.rem(b, 2)
        load2(b, s).wait()

        @pl.when(b == n_b2 - 1)
        def _():
            for k in range(4):
                sb_copy(0, k, 0, n_b2 - 1, slot).start()

        want = jnp.broadcast_to(dv[:, pl.ds(pl.multiple_of(b * R2, R2), R2)] - base, (8, R2))

        def tile(j, st):
            @pl.when(jnp.logical_and(j == 0, 2 * b + 3 < n_pc))
            def _():
                got_y(2 * b + 3)

            @pl.when(jnp.logical_and(j == 1, 2 * b + 2 < n_pc))
            def _():
                got_x(2 * b + 2)

            @pl.when(jnp.logical_and(j == 2, 2 * b + 4 < n_pc))
            def _():
                got_y(2 * b + 4)

            @pl.when(jnp.logical_and(j == 3, 2 * b + 3 < n_pc))
            def _():
                got_x(2 * b + 3)

            @pl.when(jnp.logical_and(j == 4, b + 1 < n_b2))
            def _():
                arrived(b + 1)
                load2(b + 1, 1 - s).start()

            return score(2 * WC, j * (2 * WC), hb[s, pl.ds(0, R2), :], want, st)

        st = squeeze(lax.fori_loop(0, n_t2, tile, fresh(R2)))
        for k in range(3):
            stb[b, k:k + 1, :] = st[k]
        return carry

    lax.fori_loop(0, n_b2, block2, 0)
    for k in range(4):
        sb_copy(1, k, n_b2 - 1, 1, slot).start()

    for k in range(1, 4):
        sa_copy(k, y * 4 + peer(k)).wait_recv()
    for k in range(4):
        sb_copy(0, k, 0, n_b2 - 1, oy * 4 + peer(k)).wait_recv()
        sb_copy(1, k, n_b2 - 1, 1, oy * 4 + peer(k)).wait_recv()

    def combine(b, carry):
        tops = [sta[i, b, 0:1, :] for i in range(8)]
        top = functools.reduce(jnp.maximum, tops)
        tot = functools.reduce(jnp.add, [sta[i, b, 1:2, :] * jnp.exp(tops[i] - top) for i in range(8)])
        pick = functools.reduce(jnp.add, [sta[i, b, 2:3, :] for i in range(8)])
        at = pl.ds(pl.multiple_of(b * R2, R2), R2)
        lp = pick - (top + jnp.log(tot))
        lp_ref[:, at] = lp
        ac_ref[:, at] = jnp.minimum(1.0, jnp.exp(lp) / q_ref[:, at])
        return carry

    lax.fori_loop(0, n_b2, combine, 0)

    draft_copy.wait_send()
    start_loop(n_wc, lambda j: w_copy(j).wait_send())
    start_loop(n_rb, lambda i: x1_copy(i).wait_send())
    d1_copy(c).wait_send()
    start_loop(n_rb, lambda i: f1_copy(i, c).wait_send())

    def drain(t):
        y_copy(t).wait_send()
        x2_copy(t).wait_send()
        d2_copy(t, c).wait_send()
        f2_copy(t, c).wait_send()

    start_loop(n_pc, drain)
    for k in range(1, 4):
        sa_copy(k, slot).wait_send()
    for k in range(4):
        sb_copy(0, k, 0, n_b2 - 1, slot).wait_send()
        sb_copy(1, k, n_b2 - 1, 1, slot).wait_send()


def solution(mesh):
    def per_device(h_part, w_part, draft_loc, q_loc):
        rows, quarter = h_part.shape
        shard, half = w_part.shape
        n_wc, n_rb, n_pc, n_b2 = shard // 2 // WC, rows // R1, rows // PIECE, rows // R2
        dma = pltpu.SemaphoreType.DMA
        vmem = pl.BlockSpec(memory_space=pltpu.VMEM)
        hbm = pl.BlockSpec(memory_space=pl.ANY)
        lp, ac, _ = pl.pallas_call(
            functools.partial(_kernel, rows, quarter, shard, half),
            out_shape=(
                jax.ShapeDtypeStruct((1, rows), jnp.float32),
                jax.ShapeDtypeStruct((1, rows), jnp.float32),
                jax.ShapeDtypeStruct((2 * rows, 2 * half), jnp.bfloat16),
            ),
            in_specs=[hbm, hbm, vmem, vmem],
            out_specs=(vmem, vmem, hbm),
            scratch_shapes=[
                pltpu.VMEM((shard // 2, 2 * half), jnp.bfloat16),
                pltpu.VMEM((2, R1, 2 * half), jnp.bfloat16),
                pltpu.VMEM((1, rows), jnp.int32),
                pltpu.VMEM((n_rb, 3, 8, R1), jnp.float32),
                pltpu.VMEM((8, n_b2, 8, R2), jnp.float32),
                pltpu.VMEM((n_b2, 8, R2), jnp.float32),
                dma, dma((2, 3)), dma((2,)), dma((n_wc,)), dma((n_wc,)), dma((n_pc,)), dma((n_pc,)),
                dma((n_rb,)), dma((n_rb,)), dma, dma, dma((n_rb,)), dma((n_rb,)),
                dma((n_pc,)), dma((n_pc,)), dma((n_pc,)), dma((n_pc,)), dma((n_pc,)), dma((n_pc,)),
                dma((3,)), dma((3,)), dma((2, 4)), dma((2, 4)),
            ],
            compiler_params=pltpu.CompilerParams(collective_id=0, has_side_effects=True, vmem_limit_bytes=67043328),
        )(h_part, w_part, draft_loc.reshape(1, rows), q_loc.reshape(1, rows))
        return lp.reshape(rows), ac.reshape(rows)

    return jax.shard_map(per_device, mesh=mesh, in_specs=(P("data", "model"), P("model", "data"), P("data"), P("data")), out_specs=(P("data"), P("data")), check_vma=False)
```

```python
import functools

import jax
import jax.numpy as jnp
from jax import lax
from jax.experimental import pallas as pl
from jax.experimental.pallas import tpu as pltpu
from jax.sharding import PartitionSpec as P

MESH = pl.DeviceIdType.MESH
WC = 400
R1 = 512
PIECE = 64
R2 = 256
LANES = 128


def _kernel(rows, quarter, shard, half, h_ref, w_ref, d_ref, pick_ref, lse_ref, ha_ref,
            wv, hb, dv, st1, sta, stb, own_sem, ld_sem, d_sem, w_ss, w_rs, y_ss, y_rs,
            x1_ss, x1_rs, d1_ss, d1_rs, f1_ss, f1_rs, x2_ss, x2_rs, d2_ss, d2_rs, f2_ss, f2_rs,
            sa_ss, sa_rs, sb_ss, sb_rs):
    y = lax.axis_index("data")
    m = lax.axis_index("model")
    x = m // 2
    c = m % 2
    oy = 1 - y
    ox = 1 - x
    oc = 1 - c
    me_id = (y, m)
    dev_y = (oy, m)
    dev_x = (y, ox * 2 + c)
    dev_d = (y, x * 2 + oc)
    vocab = shard // 2
    base = m * shard + y * vocab
    n_wc = vocab // WC
    n_rb = rows // R1
    n_pc = rows // PIECE
    n_b2 = rows // R2

    def col(p):
        return pl.ds(pl.multiple_of(p * quarter, 128), quarter)

    def whalf(hh):
        return pl.ds(pl.multiple_of(lax.rem(hh + x, 2) * half, 128), half)

    def peer(k):
        kx, kc = k // 2, k % 2
        return lax.rem(x + kx, 2) * 2 + lax.rem(c + kc, 2)

    bar = pltpu.get_barrier_semaphore()
    for dy in range(2):
        for k in range(4):
            if dy or k:
                pl.semaphore_signal(bar, 1, device_id=(lax.rem(y + dy, 2), peer(k)), device_id_type=MESH)
    pl.semaphore_wait(bar, 7)

    def rcopy(src, dst, ss, rs, dev):
        return pltpu.make_async_remote_copy(src, dst, ss, rs, device_id=dev, device_id_type=MESH)

    def w_copy(j):
        return rcopy(w_ref.at[pl.ds(pl.multiple_of(oy * vocab + j * WC, 16), WC)],
                     wv.at[pl.ds(pl.multiple_of(j * WC, 16), WC), whalf(y)], w_ss.at[j], w_rs.at[j], dev_y)

    def w_wait(j):
        rcopy(w_ref.at[pl.ds(0, WC)], wv.at[pl.ds(pl.multiple_of(j * WC, 16), WC), whalf(oy)],
              w_ss.at[j], w_rs.at[j], dev_y).wait_recv()

    def prow(yy, t):
        return pl.ds(pl.multiple_of(yy * rows + t * PIECE, PIECE), PIECE)

    def y_copy(t):
        return rcopy(h_ref.at[pl.ds(pl.multiple_of(t * PIECE, PIECE), PIECE)], ha_ref.at[prow(y, t), col(c)],
                     y_ss.at[t], y_rs.at[t], dev_y)

    def y_wait(t):
        rcopy(h_ref.at[pl.ds(0, PIECE)], ha_ref.at[prow(oy, t), col(c)], y_ss.at[t], y_rs.at[t], dev_y).wait_recv()

    def rrow(i):
        return pl.ds(pl.multiple_of(y * rows + i * R1, R1), R1)

    def x1_copy(i):
        return rcopy(h_ref.at[pl.ds(pl.multiple_of(i * R1, R1), R1)], ha_ref.at[rrow(i), col(2 + c)],
                     x1_ss.at[i], x1_rs.at[i], dev_x)

    def d1_copy(pos):
        return rcopy(h_ref, ha_ref.at[pl.ds(pl.multiple_of(y * rows, R1), rows), col(pos)],
                     d1_ss, d1_rs, dev_d)

    def f1_copy(i, pos):
        return rcopy(ha_ref.at[rrow(i), col(2 + c)], ha_ref.at[rrow(i), col(2 + pos)],
                     f1_ss.at[i], f1_rs.at[i], dev_d)

    def x2_copy(t):
        return rcopy(ha_ref.at[prow(oy, t), col(c)], ha_ref.at[prow(oy, t), col(2 + c)],
                     x2_ss.at[t], x2_rs.at[t], dev_x)

    def d2_copy(t, pos):
        return rcopy(ha_ref.at[prow(oy, t), col(c)], ha_ref.at[prow(oy, t), col(pos)],
                     d2_ss.at[t], d2_rs.at[t], dev_d)

    def f2_copy(t, pos):
        return rcopy(ha_ref.at[prow(oy, t), col(2 + c)], ha_ref.at[prow(oy, t), col(2 + pos)],
                     f2_ss.at[t], f2_rs.at[t], dev_d)

    def got_y(t, when=True):
        @pl.when(when)
        def _():
            y_wait(t)
            x2_copy(t).start()
            d2_copy(t, c).start()

    def got_x(t, when=True):
        @pl.when(when)
        def _():
            x2_copy(t).wait_recv()
            f2_copy(t, c).start()

    def drain(t):
        y_copy(t).wait_send()
        x2_copy(t).wait_send()
        d2_copy(t, c).wait_send()
        f2_copy(t, c).wait_send()

    def start_loop(n, f):
        lax.fori_loop(0, n, lambda i, s: (f(i), s)[1], 0)

    own_w = pltpu.make_async_copy(w_ref.at[pl.ds(pl.multiple_of(y * vocab, 16), vocab)], wv.at[:, whalf(y)], own_sem)
    draft_copy = rcopy(d_ref, dv, d_sem.at[0], d_sem.at[1], dev_y)
    draft_copy.start()
    start_loop(n_wc, lambda j: w_copy(j).start())
    start_loop(n_rb, lambda i: x1_copy(i).start())
    d1_copy(c).start()
    own_w.start()

    def pass_on(i):
        x1_copy(i).wait_recv()
        f1_copy(i, c).start()

    start_loop(n_rb, pass_on)
    d1_copy(oc).wait_recv()
    start_loop(n_rb, lambda i: f1_copy(i, oc).wait_recv())

    def load1(i, s):
        r = pl.ds(pl.multiple_of(i * R1, R1), R1)
        return (
            pltpu.make_async_copy(h_ref.at[r], hb.at[s, :, col(c)], ld_sem.at[s, 0]),
            pltpu.make_async_copy(ha_ref.at[rrow(i), col(oc)], hb.at[s, :, col(oc)], ld_sem.at[s, 1]),
            pltpu.make_async_copy(ha_ref.at[rrow(i), pl.ds(half, half)], hb.at[s, :, pl.ds(half, half)], ld_sem.at[s, 2]),
        )

    def load2(b, s):
        r = pl.ds(pl.multiple_of(oy * rows + b * R2, R2), R2)
        return pltpu.make_async_copy(ha_ref.at[r], hb.at[s, pl.ds(0, R2)], ld_sem.at[s, 0])

    def score(t, v0, hblk, want, st):
        mx, sm, pk = st
        n = want.shape[1]
        wt = wv[pl.ds(pl.multiple_of(v0, 16), t), :]
        lg = lax.dot_general(wt, hblk, (((1,), (1,)), ((), ())), preferred_element_type=jnp.float32)
        lg = lg.reshape(t // 8, 8, n)
        new = jnp.maximum(mx, jnp.max(lg, axis=0))
        sm = sm * jnp.exp(mx - new) + jnp.sum(jnp.exp(lg - new[None]), axis=0)
        ids = lax.broadcasted_iota(jnp.int32, (t // 8, 8, n), 0) * 8 + lax.broadcasted_iota(jnp.int32, (t // 8, 8, n), 1)
        pk = pk + jnp.sum(jnp.where(ids == (want - v0)[None], lg, 0.0), axis=0)
        return new, sm, pk

    def fresh(n):
        return jnp.full((8, n), -jnp.inf, jnp.float32), jnp.zeros((8, n), jnp.float32), jnp.zeros((8, n), jnp.float32)

    def squeeze(st):
        mx, sm, pk = st
        top = jnp.max(mx, axis=0, keepdims=True)
        return top, jnp.sum(sm * jnp.exp(mx - top), axis=0, keepdims=True), jnp.sum(pk, axis=0, keepdims=True)

    def step1(t, v0, i, s):
        @pl.when(v0 == 0)
        def _():
            for k, a in enumerate(fresh(R1)):
                st1[i, k] = a

        want = jnp.broadcast_to(d_ref[:, pl.ds(pl.multiple_of(i * R1, R1), R1)] - base, (8, R1))
        st = score(t, v0, hb[s], want, (st1[i, 0], st1[i, 1], st1[i, 2]))
        for k in range(3):
            st1[i, k] = st[k]

    def fetch1(i, s, last):
        nxt = lax.rem(i + 1, n_rb)

        @pl.when(jnp.logical_not(last))
        def _():
            for cp in load1(nxt, 1 - s):
                cp.start()

        for cp in load1(i, s):
            cp.wait()

    n_pair = (n_wc - 2) // 2
    for cp in load1(0, 0):
        cp.start()
    own_w.wait()

    def pairs(n, carry):
        j, i, s = n // n_rb, lax.rem(n, n_rb), lax.rem(n, 2)

        @pl.when(n == n_pair * n_rb // 2)
        def _():
            start_loop(n_pc, lambda t: y_copy(t).start())

        @pl.when(i == 0)
        def _():
            w_wait(2 * j)
            w_wait(2 * j + 1)

        fetch1(i, s, False)
        step1(2 * WC, j * (2 * WC), i, s)
        return carry

    lax.fori_loop(0, n_pair * n_rb, pairs, 0)

    def singles(n, carry):
        j, i, s = 2 * n_pair + n // n_rb, lax.rem(n, n_rb), lax.rem(n, 2)

        @pl.when(i == 0)
        def _():
            w_wait(j)

        for at, ys, xs in ((1, (0,), ()), (3, (1,), ()), (4, (2,), (0,)), (6, (3,), (1,)), (7, (4,), (2,))):
            @pl.when(n == n_rb + at)
            def _():
                for t in ys:
                    got_y(t)
                for t in xs:
                    got_x(t)

        fetch1(i, s, n == 2 * n_rb - 1)
        step1(WC, j * WC, i, s)
        return carry

    lax.fori_loop(0, 2 * n_rb, singles, 0)
    got_y(5)
    got_x(3)

    slot = y * 4 + m

    def final1(i, carry):
        st = squeeze((st1[i, 0], st1[i, 1], st1[i, 2]))
        for u in range(R1 // LANES):
            for k in range(3):
                sta[slot, k, pl.ds(i * (R1 // LANES) + u, 1), :] = st[k][:, u * LANES:(u + 1) * LANES]
        return carry

    lax.fori_loop(0, n_rb, final1, 0)

    draft_copy.wait_recv()
    start_loop(n_wc, lambda j: w_copy(j).wait_send())
    start_loop(n_rb, lambda i: x1_copy(i).wait_send())
    d1_copy(c).wait_send()
    start_loop(n_rb, lambda i: f1_copy(i, c).wait_send())

    def sa_copy(k, sl):
        return rcopy(sta.at[sl], sta.at[sl], sa_ss.at[k - 1], sa_rs.at[k - 1], (y, peer(k)))

    for k in range(1, 4):
        sa_copy(k, slot).start()

    def arrived(b):
        for u in range(R2 // PIECE):
            t = b * (R2 // PIECE) + u
            d2_copy(t, oc).wait_recv()
            f2_copy(t, oc).wait_recv()

    arrived(0)
    load2(0, 0).start()

    parts = (pl.ds(0, rows // LANES - 8), pl.ds(rows // LANES - 8, 8))

    def sb_copy(g, k, sl):
        return rcopy(stb.at[:, parts[g]], sta.at[sl, :, parts[g]], sb_ss.at[g, k], sb_rs.at[g, k], (oy, peer(k)))

    n_t2 = vocab // (2 * WC)

    def block2(b, carry):
        s = lax.rem(b, 2)
        got_x(4 * b + 4, 4 * b + 4 < n_pc)
        got_y(4 * b + 6, 4 * b + 6 < n_pc)
        load2(b, s).wait()

        @pl.when(b == n_b2 - 2)
        def _():
            for k in range(4):
                sb_copy(0, k, slot).start()

        @pl.when(b >= 4)
        def _():
            for u in range(R2 // PIECE):
                drain((b - 4) * (R2 // PIECE) + u)

        want = jnp.broadcast_to(dv[:, pl.ds(pl.multiple_of(b * R2, R2), R2)] - base, (8, R2))

        def tile(j, st):
            more = b + 1 < n_b2
            got_x(4 * b + 5, jnp.logical_and(j == 1, more))
            got_y(4 * b + 7, jnp.logical_and(j == 1, more))
            got_x(4 * b + 6, jnp.logical_and(j == 2, more))
            got_y(4 * b + 8, jnp.logical_and(j == 2, 4 * b + 8 < n_pc))
            got_x(4 * b + 7, jnp.logical_and(j == 3, more))
            got_y(4 * b + 9, jnp.logical_and(j == 3, 4 * b + 9 < n_pc))

            @pl.when(jnp.logical_and(j == 4, more))
            def _():
                arrived(b + 1)
                load2(b + 1, 1 - s).start()

            return score(2 * WC, j * (2 * WC), hb[s, pl.ds(0, R2), :], want, st)

        st = squeeze(lax.fori_loop(0, n_t2, tile, fresh(R2)))
        for u in range(R2 // LANES):
            for k in range(3):
                stb[k, pl.ds(b * (R2 // LANES) + u, 1), :] = st[k][:, u * LANES:(u + 1) * LANES]
        return carry

    lax.fori_loop(0, n_b2, block2, 0)

    draft_copy.wait_send()
    for u in range(4 * (R2 // PIECE)):
        drain((n_b2 - 4) * (R2 // PIECE) + u)
    for k in range(1, 4):
        sa_copy(k, slot).wait_send()
        sa_copy(k, y * 4 + peer(k)).wait_recv()
    for k in range(4):
        sb_copy(0, k, slot).wait_send()
        sb_copy(0, k, oy * 4 + peer(k)).wait_recv()
    for k in range(4):
        sb_copy(1, k, slot).start()
    for k in range(4):
        sb_copy(1, k, oy * 4 + peer(k)).wait_recv()

    tops = [sta[i, 0] for i in range(8)]
    top = functools.reduce(jnp.maximum, tops)
    tot = functools.reduce(jnp.add, [sta[i, 1] * jnp.exp(tops[i] - top) for i in range(8)])
    lse_ref[...] = top + jnp.log(tot)
    pick_ref[...] = functools.reduce(jnp.add, [sta[i, 2] for i in range(8)])
    for k in range(4):
        sb_copy(1, k, slot).wait_send()


def solution(mesh):
    def per_device(h_part, w_part, draft_loc, q_loc):
        rows, quarter = h_part.shape
        shard, half = w_part.shape
        n_wc, n_rb, n_pc = shard // 2 // WC, rows // R1, rows // PIECE
        dma = pltpu.SemaphoreType.DMA
        vmem = pl.BlockSpec(memory_space=pltpu.VMEM)
        hbm = pl.BlockSpec(memory_space=pl.ANY)
        pick, lse, _ = pl.pallas_call(
            functools.partial(_kernel, rows, quarter, shard, half),
            out_shape=(
                jax.ShapeDtypeStruct((rows // LANES, LANES), jnp.float32),
                jax.ShapeDtypeStruct((rows // LANES, LANES), jnp.float32),
                jax.ShapeDtypeStruct((2 * rows, 2 * half), jnp.bfloat16),
            ),
            in_specs=[hbm, hbm, vmem],
            out_specs=(vmem, vmem, hbm),
            scratch_shapes=[
                pltpu.VMEM((shard // 2, 2 * half), jnp.bfloat16),
                pltpu.VMEM((2, R1, 2 * half), jnp.bfloat16),
                pltpu.VMEM((1, rows), jnp.int32),
                pltpu.VMEM((n_rb, 3, 8, R1), jnp.float32),
                pltpu.VMEM((8, 3, rows // LANES, LANES), jnp.float32),
                pltpu.VMEM((3, rows // LANES, LANES), jnp.float32),
                dma, dma((2, 3)), dma((2,)), dma((n_wc,)), dma((n_wc,)), dma((n_pc,)), dma((n_pc,)),
                dma((n_rb,)), dma((n_rb,)), dma, dma, dma((n_rb,)), dma((n_rb,)),
                dma((n_pc,)), dma((n_pc,)), dma((n_pc,)), dma((n_pc,)), dma((n_pc,)), dma((n_pc,)),
                dma((3,)), dma((3,)), dma((2, 4)), dma((2, 4)),
            ],
            compiler_params=pltpu.CompilerParams(collective_id=0, has_side_effects=True, vmem_limit_bytes=67043328),
        )(h_part, w_part, draft_loc.reshape(1, rows))
        log_prob = pick.reshape(rows) - lse.reshape(rows)
        return log_prob, jnp.minimum(1.0, jnp.exp(log_prob) / q_loc)

    return jax.shard_map(per_device, mesh=mesh, in_specs=(P("data", "model"), P("model", "data"), P("data"), P("data")), out_specs=(P("data"), P("data")), check_vma=False)
```

```python
import functools

import jax
import jax.numpy as jnp
from jax import lax
from jax.experimental import pallas as pl
from jax.experimental.pallas import tpu as pltpu
from jax.sharding import PartitionSpec as P

MESH = pl.DeviceIdType.MESH
WT = 752
WL = 240
RX = 512
PIECE = 64
R = 256
LANES = 128
PIECE_T, HOP_T, STEP1_T, STEP2_T, START2_T, SLACK_T = 350, 900, 250, 256, 4500, 30


def _kernel(rows, quarter, shard, half, h_ref, w_ref, d_ref, pick_ref, lse_ref, ha_ref,
            wv, hb, part, dv, st, sta, stb, own_sem, ld_sem, d_sem, w_ss, w_rs, y_ss, y_rs,
            x1_ss, x1_rs, d1_ss, d1_rs, f1_ss, f1_rs, x2_ss, x2_rs, d2_ss, d2_rs, f2_ss, f2_rs,
            sa_ss, sa_rs, sb_ss, sb_rs):
    y = lax.axis_index("data")
    m = lax.axis_index("model")
    x = m // 2
    c = m % 2
    oy = 1 - y
    dev_y = (oy, m)
    dev_x = (y, (1 - x) * 2 + c)
    dev_d = (y, x * 2 + 1 - c)
    vocab = shard // 2
    base = m * shard + y * vocab
    n_wt = (vocab - WL) // WT
    vl = n_wt * WT
    n_x1 = rows // RX
    n_pc = rows // PIECE
    n_b = rows // R

    def col(p):
        return pl.ds(pl.multiple_of(p * quarter, 128), quarter)

    xy = lax.rem(x + y, 2)
    mine = xy * 2 + c
    core = xy * 2 + 1 - c
    far = (1 - xy) * 2 + c
    farcore = (1 - xy) * 2 + 1 - c
    own_cols, other_cols = pl.ds(0, half), pl.ds(half, half)

    def peer(k):
        kx, kc = k // 2, k % 2
        return lax.rem(x + kx, 2) * 2 + lax.rem(c + kc, 2)

    bar = pltpu.get_barrier_semaphore()
    for dy in range(2):
        for k in range(4):
            if dy or k:
                pl.semaphore_signal(bar, 1, device_id=(lax.rem(y + dy, 2), peer(k)), device_id_type=MESH)
    pl.semaphore_wait(bar, 7)

    def rcopy(src, dst, ss, rs, dev):
        return pltpu.make_async_remote_copy(src, dst, ss, rs, device_id=dev, device_id_type=MESH)

    def rds(start, n, to=16):
        return pl.ds(pl.multiple_of(start, to), n)

    def w_copy(j):
        return rcopy(w_ref.at[rds(oy * vocab + j * WT, WT)], wv.at[rds(j * WT, WT), other_cols],
                     w_ss.at[j], w_rs.at[j], dev_y)

    wl_copy = rcopy(w_ref.at[rds(oy * vocab + vl, WL)], wv.at[pl.ds(vl, WL), other_cols],
                    w_ss.at[n_wt], w_rs.at[n_wt], dev_y)

    def prow(yy, t):
        return rds(yy * rows + t * PIECE, PIECE, PIECE)

    def y_copy(t):
        return rcopy(h_ref.at[rds(t * PIECE, PIECE, PIECE)], ha_ref.at[prow(y, t), col(far)],
                     y_ss.at[t], y_rs.at[t], dev_y)

    def y_wait(t):
        rcopy(h_ref.at[pl.ds(0, PIECE)], ha_ref.at[prow(oy, t), col(mine)], y_ss.at[t], y_rs.at[t], dev_y).wait_recv()

    def rrow(i):
        return rds(y * rows + i * RX, RX, RX)

    def x1_copy(i, pos):
        return rcopy(h_ref.at[rds(i * RX, RX, RX)], ha_ref.at[rrow(i), col(pos)], x1_ss.at[i], x1_rs.at[i], dev_x)

    def d1_copy(pos):
        return rcopy(h_ref, ha_ref.at[rds(y * rows, rows, RX), col(pos)], d1_ss, d1_rs, dev_d)

    def f1_copy(i, pos):
        return rcopy(ha_ref.at[rrow(i), col(far)], ha_ref.at[rrow(i), col(pos)], f1_ss.at[i], f1_rs.at[i], dev_d)

    def x2_copy(t, pos):
        return rcopy(ha_ref.at[prow(oy, t), col(mine)], ha_ref.at[prow(oy, t), col(pos)],
                     x2_ss.at[t], x2_rs.at[t], dev_x)

    def d2_copy(t, pos):
        return rcopy(ha_ref.at[prow(oy, t), col(mine)], ha_ref.at[prow(oy, t), col(pos)],
                     d2_ss.at[t], d2_rs.at[t], dev_d)

    def f2_copy(t, pos):
        return rcopy(ha_ref.at[prow(oy, t), col(far)], ha_ref.at[prow(oy, t), col(pos)],
                     f2_ss.at[t], f2_rs.at[t], dev_d)

    def got_y(t):
        y_wait(t)
        x2_copy(t, mine).start()
        d2_copy(t, mine).start()

    def got_x(t):
        x2_copy(t, far).wait_recv()
        f2_copy(t, far).start()

    def drain(t):
        y_copy(t).wait_send()
        x2_copy(t, mine).wait_send()
        d2_copy(t, mine).wait_send()
        f2_copy(t, far).wait_send()

    def span(lo, hi, f):
        lax.fori_loop(lo, hi, lambda i, s: (f(i), s)[1], 0)

    def due(now, least):
        ny = jnp.minimum(n_pc, jnp.maximum((now + SLACK_T) // PIECE_T, least))
        nx = jnp.minimum(n_pc, jnp.maximum(jnp.maximum(now - HOP_T, 0) // PIECE_T, least))
        return ny, nx

    def pass_pieces(before, after):
        span(before[0], after[0], got_y)
        span(before[1], after[1], got_x)

    own_w = pltpu.make_async_copy(w_ref.at[rds(y * vocab, vocab)], wv.at[:, own_cols], own_sem)
    draft_copy = rcopy(d_ref, dv, d_sem.at[0], d_sem.at[1], dev_y)
    draft_copy.start()
    span(0, n_wt, lambda j: w_copy(j).start())
    span(0, n_x1, lambda i: x1_copy(i, mine).start())
    d1_copy(mine).start()
    own_w.start()

    def own_in(i):
        s = lax.rem(i, 4)
        return pltpu.make_async_copy(h_ref.at[rds(i * R, R, R)], hb.at[s, :, pl.ds(0, quarter)], ld_sem.at[s, 0])

    def own_out(i):
        s = lax.rem(i, 4)
        return pltpu.make_async_copy(hb.at[s, :, pl.ds(0, quarter)], ha_ref.at[rds(y * rows + i * R, R, R), col(mine)], ld_sem.at[s, 1])

    def own_step(i):
        @pl.when(i >= 4)
        def _():
            own_out(i - 4).wait()

        @pl.when(i < n_b)
        def _():
            own_in(i).start()
            own_in(i).wait()
            own_out(i).start()

    span(0, n_b + 4, own_step)

    def pass_on(i):
        x1_copy(i, far).wait_recv()
        f1_copy(i, far).start()

    span(0, n_x1, pass_on)
    d1_copy(core).wait_recv()
    span(0, n_x1, lambda i: f1_copy(i, farcore).wait_recv())
    own_w.wait()

    def load(yy, i, s):
        return pltpu.make_async_copy(ha_ref.at[rds(yy * rows + i * R, R, R)], hb.at[s], ld_sem.at[s, 0])

    def dot(a, b):
        return lax.dot_general(a, b, (((1,), (1,)), ((), ())), preferred_element_type=jnp.float32)

    def update(lg, v0, want, old):
        mx, sm, pk = old
        t = lg.shape[0]
        lg = lg.reshape(t // 8, 8, R)
        new = jnp.maximum(mx, jnp.max(lg, axis=0))
        sm = sm * jnp.exp(mx - new) + jnp.sum(jnp.exp(lg - new[None]), axis=0)
        ids = lax.broadcasted_iota(jnp.int32, (t // 8, 8, R), 0) * 8 + lax.broadcasted_iota(jnp.int32, (t // 8, 8, R), 1)
        pk = pk + jnp.sum(jnp.where(ids == (want - v0)[None], lg, 0.0), axis=0)
        return new, sm, pk

    def fresh():
        return jnp.full((8, R), -jnp.inf, jnp.float32), jnp.zeros((8, R), jnp.float32), jnp.zeros((8, R), jnp.float32)

    def first_part(b, s):
        part[b] = dot(wv[pl.ds(vl, WL), own_cols], hb[s, :, own_cols])

    load(y, 0, 0).start()

    def step1(n, carry):
        j, i, s = n // n_b, lax.rem(n, n_b), lax.rem(n, 2)

        @pl.when(n == n_b)
        def _():
            span(0, n_pc, lambda t: y_copy(t).start())
            wl_copy.start()

        @pl.when(i == 0)
        def _():
            w_copy(j).wait_recv()

        @pl.when(jnp.logical_and(j == n_wt - 1, i > 0))
        def _():
            pass_pieces(due((i - 1) * STEP1_T, 0), due(i * STEP1_T, 0))

        @pl.when(n + 1 < n_wt * n_b)
        def _():
            load(y, lax.rem(i + 1, n_b), 1 - s).start()

        load(y, i, s).wait()

        @pl.when(j == 0)
        def _():
            for k, a in enumerate(fresh()):
                st[i, k] = a
            first_part(i, s)

        want = jnp.broadcast_to(d_ref[:, rds(i * R, R, R)] - base, (8, R))
        new = update(dot(wv[rds(j * WT, WT), :], hb[s]), j * WT, want, (st[i, 0], st[i, 1], st[i, 2]))
        for k in range(3):
            st[i, k] = new[k]
        return carry

    lax.fori_loop(0, n_wt * n_b, step1, 0)

    draft_copy.wait_recv()
    span(0, n_wt, lambda j: w_copy(j).wait_send())
    span(0, n_x1, lambda i: x1_copy(i, mine).wait_send())
    d1_copy(mine).wait_send()
    span(0, n_x1, lambda i: f1_copy(i, far).wait_send())

    per = R // PIECE

    def arrived(b):
        for u in range(per):
            d2_copy(b * per + u, core).wait_recv()
            f2_copy(b * per + u, farcore).wait_recv()

    arrived(0)
    load(oy, 0, 0).start()

    def block2(b, carry):
        s = lax.rem(b, 2)
        load(oy, b, s).wait()
        first_part(n_b + b, s)
        want = jnp.broadcast_to(dv[:, rds(b * R, R, R)] - base, (8, R))

        @pl.when(b >= 4)
        def _():
            for u in range(per):
                drain((b - 4) * per + u)

        def tile(j, old):
            now = START2_T + (b * n_wt + j) * STEP2_T
            least = (b + 1) * per
            before = jnp.where(b + j == 0, (n_b - 1) * STEP1_T, now - STEP2_T)
            pass_pieces(due(before, least), due(now, least + per * (j // (n_wt - 1))))

            @pl.when(jnp.logical_and(j == n_wt - 1, b + 1 < n_b))
            def _():
                arrived(b + 1)
                load(oy, b + 1, 1 - s).start()

            return update(dot(wv[rds(j * WT, WT), :], hb[s]), j * WT, want, old)

        new = lax.fori_loop(0, n_wt, tile, fresh())
        for k in range(3):
            st[n_b + b, k] = new[k]
        return carry

    lax.fori_loop(0, n_b, block2, 0)

    n_g = n_b // 2

    def load_pair(g):
        s = lax.rem(g, 4)
        r = lax.rem(oy + g // n_g, 2) * rows + lax.rem(g, n_g) * (2 * R)
        return [pltpu.make_async_copy(ha_ref.at[rds(r + u * R, R, R), other_cols], hb.at[s, :, pl.ds(u * half, half)],
                                      ld_sem.at[s, u]) for u in range(2)]

    for g in range(3):
        for cp in load_pair(g):
            cp.start()
    for u in range(4 * per):
        drain((n_b - 4) * per + u)
    draft_copy.wait_send()

    slot = y * 4 + m
    n_row = rows // LANES
    parts = (pl.ds(0, n_row - 8), pl.ds(n_row - 8, 8))

    def sb_copy(k, sl):
        return rcopy(stb, sta.at[sl], sb_ss.at[k], sb_rs.at[k], (oy, peer(k)))

    def sa_copy(g, k, sl):
        return rcopy(sta.at[sl, :, parts[g]], sta.at[sl, :, parts[g]], sa_ss.at[g, k - 1], sa_rs.at[g, k - 1], (y, peer(k)))

    def last(g, first, ids_ref, out):
        s = lax.rem(g, 4)

        @pl.when(g + 3 < 2 * n_g)
        def _():
            for cp in load_pair(g + 3):
                cp.start()

        for cp in load_pair(g):
            cp.wait()
        w = wv[pl.ds(vl, WL), other_cols]
        for u in range(2):
            i = lax.rem(g, n_g) * 2 + u
            b = first + i
            want = jnp.broadcast_to(ids_ref[:, rds(i * R, R, R)] - base, (8, R))
            lg = part[b] + dot(w, hb[s, :, u * half:(u + 1) * half])
            mx, sm, pk = update(lg, vl, want, (st[b, 0], st[b, 1], st[b, 2]))
            top = jnp.max(mx, axis=0, keepdims=True)
            res = (top, jnp.sum(sm * jnp.exp(mx - top), axis=0, keepdims=True), jnp.sum(pk, axis=0, keepdims=True))
            for v in range(R // LANES):
                for k in range(3):
                    out[k, pl.ds(i * (R // LANES) + v, 1), :] = res[k][:, v * LANES:(v + 1) * LANES]

    wl_copy.wait_recv()
    span(0, n_g, lambda g: last(g, n_b, dv, stb))

    def last_own(g):
        @pl.when(g == n_g + 1)
        def _():
            for k in range(4):
                sb_copy(k, slot).start()

        @pl.when(g == 2 * n_g - 1)
        def _():
            for k in range(1, 4):
                sa_copy(0, k, slot).start()

        last(g, 0, d_ref, sta.at[slot])

    span(n_g, 2 * n_g, last_own)

    wl_copy.wait_send()
    for k in range(4):
        sb_copy(k, slot).wait_send()
        sb_copy(k, oy * 4 + peer(k)).wait_recv()
    for k in range(1, 4):
        sa_copy(1, k, slot).start()
    for g in range(2):
        for k in range(1, 4):
            sa_copy(g, k, y * 4 + peer(k)).wait_recv()

    tops = [sta[i, 0] for i in range(8)]
    top = functools.reduce(jnp.maximum, tops)
    tot = functools.reduce(jnp.add, [sta[i, 1] * jnp.exp(tops[i] - top) for i in range(8)])
    lse_ref[...] = top + jnp.log(tot)
    pick_ref[...] = functools.reduce(jnp.add, [sta[i, 2] for i in range(8)])
    for g in range(2):
        for k in range(1, 4):
            sa_copy(g, k, slot).wait_send()


def solution(mesh):
    def per_device(h_part, w_part, draft_loc, q_loc):
        rows, quarter = h_part.shape
        shard, half = w_part.shape
        n_w, n_x1, n_pc, n_b = (shard // 2 - WL) // WT + 1, rows // RX, rows // PIECE, rows // R
        dma = pltpu.SemaphoreType.DMA
        vmem = pl.BlockSpec(memory_space=pltpu.VMEM)
        hbm = pl.BlockSpec(memory_space=pl.ANY)
        sums = jax.ShapeDtypeStruct((rows // LANES, LANES), jnp.float32)
        pick, lse, _ = pl.pallas_call(
            functools.partial(_kernel, rows, quarter, shard, half),
            out_shape=(sums, sums, jax.ShapeDtypeStruct((2 * rows, 2 * half), jnp.bfloat16)),
            in_specs=[hbm, hbm, vmem],
            out_specs=(vmem, vmem, hbm),
            scratch_shapes=[
                pltpu.VMEM((shard // 2, 2 * half), jnp.bfloat16),
                pltpu.VMEM((4, R, 2 * half), jnp.bfloat16),
                pltpu.VMEM((2 * n_b, WL, R), jnp.float32),
                pltpu.VMEM((1, rows), jnp.int32),
                pltpu.VMEM((2 * n_b, 3, 8, R), jnp.float32),
                pltpu.VMEM((8, 3, rows // LANES, LANES), jnp.float32),
                pltpu.VMEM((3, rows // LANES, LANES), jnp.float32),
                dma, dma((4, 2)), dma((2,)), dma((n_w,)), dma((n_w,)), dma((n_pc,)), dma((n_pc,)),
                dma((n_x1,)), dma((n_x1,)), dma, dma, dma((n_x1,)), dma((n_x1,)),
                dma((n_pc,)), dma((n_pc,)), dma((n_pc,)), dma((n_pc,)), dma((n_pc,)), dma((n_pc,)),
                dma((2, 3)), dma((2, 3)), dma((4,)), dma((4,)),
            ],
            compiler_params=pltpu.CompilerParams(collective_id=0, has_side_effects=True, vmem_limit_bytes=67043328),
        )(h_part, w_part, draft_loc.reshape(1, rows))
        log_prob = pick.reshape(rows) - lse.reshape(rows)
        return log_prob, jnp.minimum(1.0, jnp.exp(log_prob) / q_loc)

    return jax.shard_map(per_device, mesh=mesh, in_specs=(P("data", "model"), P("model", "data"), P("data"), P("data")), out_specs=(P("data"), P("data")), check_vma=False)
```

```python
import functools

import jax
import jax.numpy as jnp
from jax import lax
from jax.experimental import pallas as pl
from jax.experimental.pallas import tpu as pltpu
from jax.sharding import PartitionSpec as P

MESH = pl.DeviceIdType.MESH
WT = 752
WL = 240
RX = 512
PIECE = 64
R = 256
LANES = 128
PIECE_T, HOP_T, STEP1_T, STEP2_T, START2_T, SLACK_T = 350, 900, 250, 256, 4500, 30


def _kernel(rows, quarter, shard, half, h_ref, w_ref, dh_ref, pick_ref, lse_ref, ha_ref,
            wv, hb, part, d_ref, dv, st, sta, stb, own_sem, ld_sem, d_sem, w_ss, w_rs, y_ss, y_rs,
            x1_ss, x1_rs, d1_ss, d1_rs, f1_ss, f1_rs, x2_ss, x2_rs, d2_ss, d2_rs, f2_ss, f2_rs,
            sa_ss, sa_rs, sb_ss, sb_rs):
    y = lax.axis_index("data")
    m = lax.axis_index("model")
    x = m // 2
    c = m % 2
    oy = 1 - y
    dev_y = (oy, m)
    dev_x = (y, (1 - x) * 2 + c)
    dev_d = (y, x * 2 + 1 - c)
    vocab = shard // 2
    base = m * shard + y * vocab
    n_wt = (vocab - WL) // WT
    vl = n_wt * WT
    n_x1 = rows // RX
    n_pc = rows // PIECE
    n_b = rows // R

    def col(p):
        return pl.ds(pl.multiple_of(p * quarter, 128), quarter)

    xy = lax.rem(x + y, 2)
    mine = xy * 2 + c
    core = xy * 2 + 1 - c
    far = (1 - xy) * 2 + c
    farcore = (1 - xy) * 2 + 1 - c
    own_cols, other_cols = pl.ds(0, half), pl.ds(half, half)

    def peer(k):
        kx, kc = k // 2, k % 2
        return lax.rem(x + kx, 2) * 2 + lax.rem(c + kc, 2)

    bar = pltpu.get_barrier_semaphore()
    for dy in range(2):
        for k in range(4):
            if dy or k:
                pl.semaphore_signal(bar, 1, device_id=(lax.rem(y + dy, 2), peer(k)), device_id_type=MESH)
    pl.semaphore_wait(bar, 7)

    def rcopy(src, dst, ss, rs, dev):
        return pltpu.make_async_remote_copy(src, dst, ss, rs, device_id=dev, device_id_type=MESH)

    def rds(start, n, to=16):
        return pl.ds(pl.multiple_of(start, to), n)

    def w_copy(j):
        return rcopy(w_ref.at[rds(oy * vocab + j * WT, WT)], wv.at[rds(j * WT, WT), other_cols],
                     w_ss.at[j], w_rs.at[j], dev_y)

    wl_copy = rcopy(w_ref.at[rds(oy * vocab + vl, WL)], wv.at[pl.ds(vl, WL), other_cols],
                    w_ss.at[n_wt], w_rs.at[n_wt], dev_y)

    def prow(yy, t):
        return rds(yy * rows + t * PIECE, PIECE, PIECE)

    def y_copy(t):
        return rcopy(h_ref.at[rds(t * PIECE, PIECE, PIECE)], ha_ref.at[prow(y, t), col(far)],
                     y_ss.at[t], y_rs.at[t], dev_y)

    def y_wait(t):
        rcopy(h_ref.at[pl.ds(0, PIECE)], ha_ref.at[prow(oy, t), col(mine)], y_ss.at[t], y_rs.at[t], dev_y).wait_recv()

    def rrow(i):
        return rds(y * rows + i * RX, RX, RX)

    def x1_copy(i, pos):
        return rcopy(h_ref.at[rds(i * RX, RX, RX)], ha_ref.at[rrow(i), col(pos)], x1_ss.at[i], x1_rs.at[i], dev_x)

    def d1_copy(pos):
        return rcopy(h_ref, ha_ref.at[rds(y * rows, rows, RX), col(pos)], d1_ss, d1_rs, dev_d)

    def f1_copy(i, pos):
        return rcopy(ha_ref.at[rrow(i), col(far)], ha_ref.at[rrow(i), col(pos)], f1_ss.at[i], f1_rs.at[i], dev_d)

    def x2_copy(t, pos):
        return rcopy(ha_ref.at[prow(oy, t), col(mine)], ha_ref.at[prow(oy, t), col(pos)],
                     x2_ss.at[t], x2_rs.at[t], dev_x)

    def d2_copy(t, pos):
        return rcopy(ha_ref.at[prow(oy, t), col(mine)], ha_ref.at[prow(oy, t), col(pos)],
                     d2_ss.at[t], d2_rs.at[t], dev_d)

    def f2_copy(t, pos):
        return rcopy(ha_ref.at[prow(oy, t), col(far)], ha_ref.at[prow(oy, t), col(pos)],
                     f2_ss.at[t], f2_rs.at[t], dev_d)

    def got_y(t):
        y_wait(t)
        x2_copy(t, mine).start()
        d2_copy(t, mine).start()

    def got_x(t):
        x2_copy(t, far).wait_recv()
        f2_copy(t, far).start()

    def drain(t):
        y_copy(t).wait_send()
        x2_copy(t, mine).wait_send()
        d2_copy(t, mine).wait_send()
        f2_copy(t, far).wait_send()

    def span(lo, hi, f):
        lax.fori_loop(lo, hi, lambda i, s: (f(i), s)[1], 0)

    def due(now, least):
        ny = jnp.minimum(n_pc, jnp.maximum((now + SLACK_T) // PIECE_T, least))
        nx = jnp.minimum(n_pc, jnp.maximum(jnp.maximum(now - HOP_T, 0) // PIECE_T, least))
        return ny, nx

    def pass_pieces(before, after):
        span(before[0], after[0], got_y)
        span(before[1], after[1], got_x)

    own_w = pltpu.make_async_copy(w_ref.at[rds(y * vocab, vocab)], wv.at[:, own_cols], own_sem)
    draft_copy = rcopy(dh_ref, dv, d_sem.at[0], d_sem.at[1], dev_y)
    own_d = pltpu.make_async_copy(dh_ref, d_ref, d_sem.at[2])
    draft_copy.start()
    own_d.start()
    span(0, n_wt, lambda j: w_copy(j).start())
    span(0, n_x1, lambda i: x1_copy(i, mine).start())
    d1_copy(mine).start()
    own_w.start()

    def own_in(i):
        s = lax.rem(i, 4)
        return pltpu.make_async_copy(h_ref.at[rds(i * R, R, R)], hb.at[s, :, pl.ds(0, quarter)], ld_sem.at[s, 0])

    def own_out(i):
        s = lax.rem(i, 4)
        return pltpu.make_async_copy(hb.at[s, :, pl.ds(0, quarter)], ha_ref.at[rds(y * rows + i * R, R, R), col(mine)], ld_sem.at[s, 1])

    def own_step(i):
        @pl.when(i >= 4)
        def _():
            own_out(i - 4).wait()

        @pl.when(i < n_b)
        def _():
            own_in(i).start()
            own_in(i).wait()
            own_out(i).start()

    span(0, n_b + 4, own_step)

    def pass_on(i):
        x1_copy(i, far).wait_recv()
        f1_copy(i, far).start()

    span(0, n_x1, pass_on)
    d1_copy(core).wait_recv()
    span(0, n_x1, lambda i: f1_copy(i, farcore).wait_recv())
    own_w.wait()
    own_d.wait()

    def load(yy, i, s):
        return pltpu.make_async_copy(ha_ref.at[rds(yy * rows + i * R, R, R)], hb.at[s], ld_sem.at[s, 0])

    def dot(a, b):
        return lax.dot_general(a, b, (((1,), (1,)), ((), ())), preferred_element_type=jnp.float32)

    def update(lg, v0, want, old):
        mx, sm, pk = old
        t = lg.shape[0]
        lg = lg.reshape(t // 8, 8, R)
        new = jnp.maximum(mx, jnp.max(lg, axis=0))
        sm = sm * jnp.exp(mx - new) + jnp.sum(jnp.exp(lg - new[None]), axis=0)
        ids = lax.broadcasted_iota(jnp.int32, (t // 8, 8, R), 0) * 8 + lax.broadcasted_iota(jnp.int32, (t // 8, 8, R), 1)
        pk = pk + jnp.sum(jnp.where(ids == (want - v0)[None], lg, 0.0), axis=0)
        return new, sm, pk

    def fresh():
        return jnp.full((8, R), -jnp.inf, jnp.float32), jnp.zeros((8, R), jnp.float32), jnp.zeros((8, R), jnp.float32)

    def first_part(b, s):
        part[b] = dot(wv[pl.ds(vl, WL), own_cols], hb[s, :, own_cols])

    load(y, 0, 0).start()

    def step1(n, carry):
        j, i, s = n // n_b, lax.rem(n, n_b), lax.rem(n, 2)

        @pl.when(n == n_b)
        def _():
            span(0, n_pc, lambda t: y_copy(t).start())
            wl_copy.start()

        @pl.when(i == 0)
        def _():
            w_copy(j).wait_recv()

        @pl.when(jnp.logical_and(j == n_wt - 1, i > 0))
        def _():
            pass_pieces(due((i - 1) * STEP1_T, 0), due(i * STEP1_T, 0))

        @pl.when(n + 1 < n_wt * n_b)
        def _():
            load(y, lax.rem(i + 1, n_b), 1 - s).start()

        load(y, i, s).wait()

        @pl.when(j == 0)
        def _():
            for k, a in enumerate(fresh()):
                st[i, k] = a
            first_part(i, s)

        want = jnp.broadcast_to(d_ref[:, rds(i * R, R, R)] - base, (8, R))
        new = update(dot(wv[rds(j * WT, WT), :], hb[s]), j * WT, want, (st[i, 0], st[i, 1], st[i, 2]))
        for k in range(3):
            st[i, k] = new[k]
        return carry

    lax.fori_loop(0, n_wt * n_b, step1, 0)

    draft_copy.wait_recv()
    span(0, n_wt, lambda j: w_copy(j).wait_send())
    span(0, n_x1, lambda i: x1_copy(i, mine).wait_send())
    d1_copy(mine).wait_send()
    span(0, n_x1, lambda i: f1_copy(i, far).wait_send())

    per = R // PIECE

    def arrived(b):
        for u in range(per):
            d2_copy(b * per + u, core).wait_recv()
            f2_copy(b * per + u, farcore).wait_recv()

    arrived(0)
    load(oy, 0, 0).start()

    def block2(b, carry):
        s = lax.rem(b, 2)
        load(oy, b, s).wait()
        first_part(n_b + b, s)
        want = jnp.broadcast_to(dv[:, rds(b * R, R, R)] - base, (8, R))

        @pl.when(b >= 4)
        def _():
            for u in range(per):
                drain((b - 4) * per + u)

        def tile(j, old):
            now = START2_T + (b * n_wt + j) * STEP2_T
            least = (b + 1) * per
            before = jnp.where(b + j == 0, (n_b - 1) * STEP1_T, now - STEP2_T)
            pass_pieces(due(before, least), due(now, least + per * (j // (n_wt - 1))))

            @pl.when(jnp.logical_and(j == n_wt - 1, b + 1 < n_b))
            def _():
                arrived(b + 1)
                load(oy, b + 1, 1 - s).start()

            return update(dot(wv[rds(j * WT, WT), :], hb[s]), j * WT, want, old)

        new = lax.fori_loop(0, n_wt, tile, fresh())
        for k in range(3):
            st[n_b + b, k] = new[k]
        return carry

    lax.fori_loop(0, n_b, block2, 0)

    n_g = n_b // 2

    def load_pair(g):
        s = lax.rem(g, 4)
        r = lax.rem(oy + g // n_g, 2) * rows + lax.rem(g, n_g) * (2 * R)
        return [pltpu.make_async_copy(ha_ref.at[rds(r + u * R, R, R), other_cols], hb.at[s, :, pl.ds(u * half, half)],
                                      ld_sem.at[s, u]) for u in range(2)]

    for g in range(3):
        for cp in load_pair(g):
            cp.start()
    for u in range(4 * per):
        drain((n_b - 4) * per + u)
    draft_copy.wait_send()

    slot = y * 4 + m
    n_eight = n_b // 8

    def sb_copy(k, sl):
        return rcopy(stb, sta.at[sl], sb_ss.at[k], sb_rs.at[k], (oy, peer(k)))

    def sa_copy(g, k, sl):
        eight = sta.at[sl, :, :, pl.ds(g * 8, 8)]
        return rcopy(eight, eight, sa_ss.at[g, k - 1], sa_rs.at[g, k - 1], (y, peer(k)))

    def squeeze(b, out, g):
        mx, sm, pk = (st[pl.ds(b, 8), k] for k in range(3))
        top = jnp.max(mx, axis=1)
        res = (top, jnp.sum(sm * jnp.exp(mx - top[:, None]), axis=1), jnp.sum(pk, axis=1))
        for k in range(3):
            for v in range(R // LANES):
                out[k, v, pl.ds(g * 8, 8), :] = res[k][:, v * LANES:(v + 1) * LANES]

    def last(g, first, ids_ref):
        s = lax.rem(g, 4)

        @pl.when(g + 3 < 2 * n_g)
        def _():
            for cp in load_pair(g + 3):
                cp.start()

        for cp in load_pair(g):
            cp.wait()
        w = wv[pl.ds(vl, WL), other_cols]
        i = lax.rem(g, n_g) * 2
        lgs = [part[first + i + u] + dot(w, hb[s, :, u * half:(u + 1) * half]) for u in range(2)]
        olds = [tuple(st[first + i + u, k] for k in range(3)) for u in range(2)]
        wants = [jnp.broadcast_to(ids_ref[:, rds((i + u) * R, R, R)] - base, (8, R)) for u in range(2)]
        news = [update(lgs[u], vl, wants[u], olds[u]) for u in range(2)]
        for u in range(2):
            for k in range(3):
                st[first + i + u, k] = news[u][k]

    wl_copy.wait_recv()
    span(0, n_g, lambda g: last(g, n_b, dv))
    for g in range(n_eight):
        squeeze(n_b + g * 8, stb, g)

    def last_own(g):
        @pl.when(g == n_g + 1)
        def _():
            for k in range(4):
                sb_copy(k, slot).start()

        @pl.when(g == 2 * n_g - 4)
        def _():
            for h in range(n_eight - 1):
                squeeze(h * 8, sta.at[slot], h)

        @pl.when(g == 2 * n_g - 2)
        def _():
            for h in range(n_eight - 1):
                for k in range(1, 4):
                    sa_copy(h, k, slot).start()

        last(g, 0, d_ref)

    span(n_g, 2 * n_g, last_own)
    squeeze((n_eight - 1) * 8, sta.at[slot], n_eight - 1)

    wl_copy.wait_send()
    for k in range(4):
        sb_copy(k, slot).wait_send()
        sb_copy(k, oy * 4 + peer(k)).wait_recv()
    for k in range(1, 4):
        sa_copy(n_eight - 1, k, slot).start()
    for g in range(n_eight):
        for k in range(1, 4):
            sa_copy(g, k, y * 4 + peer(k)).wait_recv()

    tops = [sta[i, 0] for i in range(8)]
    top = functools.reduce(jnp.maximum, tops)
    tot = functools.reduce(jnp.add, [sta[i, 1] * jnp.exp(tops[i] - top) for i in range(8)])
    lse = top + jnp.log(tot)
    pick = functools.reduce(jnp.add, [sta[i, 2] for i in range(8)])
    for i in range(n_b):
        for v in range(R // LANES):
            r = i * (R // LANES) + v
            lse_ref[r:r + 1, :] = lse[v, i:i + 1, :]
            pick_ref[r:r + 1, :] = pick[v, i:i + 1, :]
    for g in range(n_eight):
        for k in range(1, 4):
            sa_copy(g, k, slot).wait_send()


def solution(mesh):
    def per_device(h_part, w_part, draft_loc, q_loc):
        rows, quarter = h_part.shape
        shard, half = w_part.shape
        n_w, n_x1, n_pc, n_b = (shard // 2 - WL) // WT + 1, rows // RX, rows // PIECE, rows // R
        dma = pltpu.SemaphoreType.DMA
        vmem = pl.BlockSpec(memory_space=pltpu.VMEM)
        hbm = pl.BlockSpec(memory_space=pl.ANY)
        sums = jax.ShapeDtypeStruct((rows // LANES, LANES), jnp.float32)
        pick, lse, _ = pl.pallas_call(
            functools.partial(_kernel, rows, quarter, shard, half),
            out_shape=(sums, sums, jax.ShapeDtypeStruct((2 * rows, 2 * half), jnp.bfloat16)),
            in_specs=[hbm, hbm, hbm],
            out_specs=(vmem, vmem, hbm),
            scratch_shapes=[
                pltpu.VMEM((shard // 2, 2 * half), jnp.bfloat16),
                pltpu.VMEM((4, R, 2 * half), jnp.bfloat16),
                pltpu.VMEM((2 * n_b, WL, R), jnp.float32),
                pltpu.VMEM((1, rows), jnp.int32),
                pltpu.VMEM((1, rows), jnp.int32),
                pltpu.VMEM((2 * n_b, 3, 8, R), jnp.float32),
                pltpu.VMEM((8, 3, R // LANES, n_b, LANES), jnp.float32),
                pltpu.VMEM((3, R // LANES, n_b, LANES), jnp.float32),
                dma, dma((4, 2)), dma((3,)), dma((n_w,)), dma((n_w,)), dma((n_pc,)), dma((n_pc,)),
                dma((n_x1,)), dma((n_x1,)), dma, dma, dma((n_x1,)), dma((n_x1,)),
                dma((n_pc,)), dma((n_pc,)), dma((n_pc,)), dma((n_pc,)), dma((n_pc,)), dma((n_pc,)),
                dma((n_b // 8, 3)), dma((n_b // 8, 3)), dma((4,)), dma((4,)),
            ],
            compiler_params=pltpu.CompilerParams(collective_id=0, has_side_effects=True, vmem_limit_bytes=67043328),
        )(h_part, w_part, draft_loc.reshape(1, rows))
        log_prob = pick.reshape(rows) - lse.reshape(rows)
        return log_prob, jnp.minimum(1.0, jnp.exp(log_prob) / q_loc)

    return jax.shard_map(per_device, mesh=mesh, in_specs=(P("data", "model"), P("model", "data"), P("data"), P("data")), out_specs=(P("data"), P("data")), check_vma=False)
```
